128 devices in a mesh: dp: 4 (over z), seq: 32 (over x, y, core).
Axes of the slice: x: 4, y: 4, z: 4, core: 2. Of those that a mesh axis runs over, the one named last changes fastest.
Arguments:
- queries: bfloat16 [4, 4096, 4096], P('dp', 'seq'), may hold values from -6 to 6
- keys: bfloat16 [4, 4096, 4096], P('dp', 'seq'), may hold values from -6 to 6
- values: bfloat16 [4, 4096, 4096], P('dp', 'seq'), may hold values from -6 to 6
- log_decay: float32 [4, 32, 4096], P('dp', None, 'seq'), may hold values from -1 to 0
- attn_grad: bfloat16 [4, 4096, 4096], P('dp', 'seq'), may hold values from -6 to 6
- norm_gain: float32 [4096], replicated, may hold values from 0.1 to 1.9
- route_ids: int32 [4, 4096, 2], P('dp', 'seq'), may hold values from 0 to 31, all different within a row; in each aligned block of 128 rows (0 to 127, 128 to 255, ..., all dimensions but the last counted through in order) at most 10 rows name the same one
- route_weights: float32 [4, 4096, 2], P('dp', 'seq'), may hold values from 0.2 to 1
- grad_exponent: int32 [32], replicated, may hold values from -2 to 2
- w_in: bfloat16 [32, 4608, 4096], P('seq', 'dp'), may hold values from -0.09375 to 0.09375
- w_out: bfloat16 [32, 4608, 4096], P('seq', 'dp'), may hold values from -0.09375 to 0.09375
Outputs:
- layer_out: bfloat16 [4, 4096, 4096], P('dp', 'seq')
- key_out: bfloat16 [4, 4096, 4096], P('dp', 'seq')
- value_out: bfloat16 [4, 4096, 4096], P('dp', 'seq')
The draws below stay inside these ranges and needn't reach their ends.
Inputs may be any that keep to these rules, and one draw needn't show every extreme that they name: `route_ids`: in each aligned block of 128 tokens (the tokens of one device) no expert is chosen by more than 10 tokens, a bound that some block reaches; a token's 2 choices differ.
All inputs are finite; a program needn't handle non-finite values.
Results may differ from the reference program's by a relative error of at most 0.019.
Values may be sent and summed in bfloat16 or wider, within the bound.
A program may use at most 320 MiB of HBM per device.

```python
import math
import jax
import jax.numpy as jnp
import numpy as np
from jax import lax

ATTENTION_HEADS = 32
HEAD = 128
D = 4096
FF = 4608
TOP = 2
TOK_DEV = 128
EXPERTS = 32
CAP = 10
SEQUENCE_LENGTH = 4096
BATCH_SEQUENCES = 4
N_DP = 4
N_SEQ = 32


def draw_log_decay(key, part):
    complete_keys = jax.random.split(key, 7)
    slow_share = 0.5
    full_shape = (BATCH_SEQUENCES, ATTENTION_HEADS, SEQUENCE_LENGTH)
    slow_heads = jax.random.uniform(complete_keys[0], (BATCH_SEQUENCES, ATTENTION_HEADS, 1)) < slow_share
    slow_rate = jnp.exp(jax.random.uniform(complete_keys[1], (BATCH_SEQUENCES, ATTENTION_HEADS, 1), minval=jnp.log(0.05), maxval=jnp.log(0.25))) * jnp.log(10.0) / SEQUENCE_LENGTH
    fast_rate = jnp.exp(jax.random.uniform(complete_keys[2], (BATCH_SEQUENCES, ATTENTION_HEADS, 1), minval=jnp.log(1.0 / 50.0), maxval=jnp.log(1.0 / 30.0)))
    stride_frequency = jnp.where(slow_heads, slow_rate, fast_rate)
    blocks = SEQUENCE_LENGTH // TOK_DEV
    accelerator_multiplier = jnp.repeat(jnp.exp(jax.random.uniform(complete_keys[3], (BATCH_SEQUENCES, ATTENTION_HEADS, blocks), minval=jnp.log(0.5), maxval=jnp.log(1.5))), TOK_DEV, axis=2)
    jaggedness = jax.random.uniform(complete_keys[4], full_shape, minval=0.5, maxval=1.5)
    position_indices = jnp.arange(SEQUENCE_LENGTH)
    spike_position = jax.random.randint(complete_keys[5], (BATCH_SEQUENCES, 1, 1, 2), 0, SEQUENCE_LENGTH)
    spike_struck = jnp.any(position_indices[None, None, :, None] == spike_position, axis=-1)
    spike_magnitude = jnp.log(jax.random.uniform(complete_keys[6], (BATCH_SEQUENCES, ATTENTION_HEADS, 1), minval=0.5, maxval=0.8))
    sampled_values = -stride_frequency * accelerator_multiplier * jaggedness + jnp.where(spike_struck, spike_magnitude, 0.0)
    return sampled_values.astype(jnp.float32)


def place_ends(result, rng, least, largest):
    index_at = [jax.random.randint(jax.random.fold_in(rng, axis), (), 0, length) for axis, length in enumerate(result.shape)]
    widest = result.shape.index(max(result.shape))
    neighbour = index_at[:widest] + [(index_at[widest] + 1) % result.shape[widest]] + index_at[widest + 1:]
    return result.at[tuple(index_at)].set(least).at[tuple(neighbour)].set(largest)


def block_scale(key, dims, pieces, least, largest):
    def one(position, blocks):
        steps = jax.random.uniform(jax.random.fold_in(jax.random.fold_in(key, 6), position), (blocks,), jnp.float32, least / len(pieces), largest / len(pieces))
        return jnp.repeat(jnp.exp(steps), dims[position] // blocks).reshape((-1,) + (1,) * (len(dims) - position - 1))

    level = one(*pieces[0])
    for cut in pieces[1:]:
        level = level * one(*cut)
    return level


def assign_block(key, own, number, rows, count, top, most, lean):
    sequence = jax.random.permutation(key, count)
    packed, ordinary = load_shares(count, rows * top, most, lean, True), load_shares(count, rows * top, most, lean, False)
    places = jnp.arange(count)

    def named(lengths, rotation):
        used = int((lengths > 0).sum())
        fixed = max(1, used // 4)
        shifted = fixed + (places - fixed + rotation * (used - fixed)) % max(1, count - fixed)
        return jnp.zeros((count,), jnp.int32).at[sequence[jnp.where(places < fixed, places, shifted)]].set(jnp.asarray(lengths, jnp.int32))

    lengths = jnp.where(number % 4 == 0, named(packed, number // 4), named(ordinary, number - number // 4 - 1))
    mixed = jax.random.permutation(jax.random.fold_in(own, 3), count)
    donor, receiver = mixed[0:count // 2 * 2:2], mixed[1:count // 2 * 2:2]
    room = jnp.minimum(lengths[donor] - 1, most - lengths[receiver]) // 2
    room = jnp.where((donor == sequence[0]) | (receiver == sequence[0]) | (lengths[receiver] == 0), 0, jnp.maximum(room, 0))
    shifted = jax.random.randint(jax.random.fold_in(own, 4), (count // 2,), 0, 1 << 20) % (room + 1)
    lengths = lengths.at[donor].add(-shifted).at[receiver].add(shifted)
    items = jnp.searchsorted(jnp.cumsum(lengths), jnp.arange(rows * top), side="right").astype(jnp.int32)
    grid = items.reshape(top, rows).T
    grid = grid[jax.random.permutation(jax.random.fold_in(own, 1), rows)]
    rotation = jax.random.randint(jax.random.fold_in(own, 2), (rows, 1), 0, top)
    return jnp.take_along_axis(grid, (jnp.arange(top)[None, :] + rotation) % top, axis=1)


def load_shares(number_of, total, bound, lean, full):
    loads = [(1 << 20) // math.isqrt(rank ** lean) + 1 for rank in range(1, number_of + 1)]
    largest = bound if full else min(bound, max(-(-total // number_of), total * loads[0] // sum(loads)))
    least = 1 if total - largest >= number_of - 1 else 0
    counts, spare = [largest] + [least] * (number_of - 1), total - largest - least * (number_of - 1)
    while spare > 0:
        candidates = [i for i in range(1, number_of) if counts[i] < largest] or [i for i in range(1, number_of) if counts[i] < bound]
        mass, budget = sum([loads[i] for i in candidates]), spare
        for i in candidates:
            more = min(bound - counts[i], max(1, budget * loads[i] // mass), spare)
            counts[i] = counts[i] + more
            spare = spare - more
    return np.array(counts)


def normal_values(key, shape, width, reach, pieces=(), kind=jnp.bfloat16):
    values = width * jax.random.normal(key, shape, jnp.float32)
    if pieces:
        values = values * block_scale(key, shape, pieces, -0.22, 0.18)
    return jnp.clip(values, -reach, reach).astype(kind)


def setup_inputs(seed: int = 0) -> dict:
    arg_keys = jax.random.split(jax.random.key(seed), 12)
    queries = normal_values(arg_keys[0], (BATCH_SEQUENCES, SEQUENCE_LENGTH, D), 1.0, 6.0, ((0, 4), (1, 32)))
    keys = normal_values(arg_keys[1], (BATCH_SEQUENCES, SEQUENCE_LENGTH, D), 1.0, 6.0, ((0, 4), (1, 32)))
    values = normal_values(arg_keys[2], (BATCH_SEQUENCES, SEQUENCE_LENGTH, D), 1.0, 6.0, ((0, 4), (1, 32)))
    log_decay = draw_log_decay(jax.random.fold_in(arg_keys[11], 71), 0)
    attn_grad = normal_values(arg_keys[4], (BATCH_SEQUENCES, SEQUENCE_LENGTH, D), 1.0, 6.0, ((0, 4), (1, 32)))
    norm_gain = jnp.clip(1.0 + 0.18 * jax.random.normal(arg_keys[5], (D,), jnp.float32), 0.1, 1.9)
    route_ids_keys = jax.random.split(jax.random.fold_in(arg_keys[6], 1), BATCH_SEQUENCES * SEQUENCE_LENGTH // TOK_DEV)
    route_ids_turns = jax.random.permutation(jax.random.fold_in(arg_keys[6], 3), BATCH_SEQUENCES * SEQUENCE_LENGTH // TOK_DEV)
    route_ids = jax.vmap(lambda own, number: assign_block(jax.random.fold_in(arg_keys[6], 2), own, number, TOK_DEV, EXPERTS, TOP, CAP, 1))(route_ids_keys, route_ids_turns).reshape((BATCH_SEQUENCES, SEQUENCE_LENGTH, TOP))
    route_weights = jnp.clip(jnp.exp(math.log(1.0) - 1.609438 * jax.random.uniform(arg_keys[7], (BATCH_SEQUENCES, SEQUENCE_LENGTH, TOP), jnp.float32) ** block_scale(arg_keys[7], (BATCH_SEQUENCES, SEQUENCE_LENGTH, TOP), ((0, 4), (1, 32)), -0.2, 0.2)), 0.2, 1.0)
    grad_exponent = place_ends(jax.random.randint(arg_keys[8], (ATTENTION_HEADS,), -2, 3), jax.random.fold_in(arg_keys[8], 1), -2, 2).astype(jnp.int32)
    w_in = normal_values(arg_keys[9], (EXPERTS, FF, D), D ** -0.5, 0.09375, ((0, 32), (1, 4)))
    w_out = normal_values(arg_keys[10], (EXPERTS, FF, D), FF ** -0.5, 0.09375, ((0, 32), (1, 4)))
    return {"queries": queries, "keys": keys, "values": values, "log_decay": log_decay, "attn_grad": attn_grad, "norm_gain": norm_gain, "route_ids": route_ids, "route_weights": route_weights, "grad_exponent": grad_exponent, "w_in": w_in, "w_out": w_out}


norm_eps = 1e-06
highest = lax.Precision.HIGHEST

def block_decays(decay_rows):
    running = jnp.cumsum(decay_rows, axis=-1)
    block_total = running[..., -1]
    position_indices = jnp.arange(TOK_DEV)
    lower_mask = position_indices[:, None] >= position_indices[None, :]
    spread = running[..., :, None] - running[..., None, :]
    weight = jnp.where(lower_mask, jnp.exp(jnp.where(lower_mask, spread, 0.0)), 0.0)
    return (running, block_total, weight)

def split_heads(stacked):
    shaped = stacked.reshape(BATCH_SEQUENCES, SEQUENCE_LENGTH // TOK_DEV, TOK_DEV, ATTENTION_HEADS, HEAD)
    return jnp.moveaxis(shaped, 1, 0)

def split_decay(log_decay):
    shaped = log_decay.reshape(BATCH_SEQUENCES, ATTENTION_HEADS, SEQUENCE_LENGTH // TOK_DEV, TOK_DEV)
    return jnp.moveaxis(shaped, 2, 0)

def join_blocks(stacked):
    return jnp.moveaxis(stacked, 0, 1).reshape(BATCH_SEQUENCES, SEQUENCE_LENGTH, ATTENTION_HEADS, HEAD)

def reverse_step(back_state, inputs):
    query_block, grad_block, decay_rows = inputs
    running, block_total, weight = block_decays(decay_rows)
    lifted = query_block.astype(jnp.float32) * jnp.exp(jnp.swapaxes(running, 1, 2))[..., None]
    back_local = jnp.einsum('bthp,bthq->bhpq', lifted, grad_block.astype(jnp.float32), precision=highest)
    new_state = jnp.exp(block_total)[..., None, None] * back_state + back_local
    return (new_state, back_state)

def forward_step(state_in, inputs):
    query_block, key_block, value_block, grad_block, decay_rows, back_in = inputs
    running, block_total, weight = block_decays(decay_rows)
    score_scale = 1.0 / HEAD
    query_wide = query_block.astype(jnp.float32)
    key_wide = key_block.astype(jnp.float32)
    value_wide = value_block.astype(jnp.float32)
    grad_wide = grad_block.astype(jnp.float32)
    head_major = jnp.swapaxes(running, 1, 2)
    tail_decay = jnp.exp(block_total[:, None, :] - head_major)[..., None]
    lead_decay = jnp.exp(head_major)[..., None]
    scores = jnp.einsum('bthp,bshp->bhts', query_wide, key_wide)
    attn_probs = (scores * weight * score_scale).astype(jnp.bfloat16)
    attention = jnp.einsum('bhts,bshp->bthp', attn_probs.astype(jnp.float32), value_wide)
    attention = attention + score_scale * lead_decay * jnp.einsum('bthp,bhpq->bthq', query_wide, state_in, precision=highest)
    local_state = jnp.einsum('bshp,bshq->bhpq', key_wide * tail_decay, value_wide, precision=highest)
    new_state = jnp.exp(block_total)[..., None, None] * state_in + local_state
    grad_probs = (jnp.einsum('bthq,bshq->bhts', grad_wide, value_wide) * weight * score_scale).astype(jnp.bfloat16)
    key_grad = jnp.einsum('bhts,bthp->bshp', grad_probs.astype(jnp.float32), query_wide)
    key_grad = key_grad + score_scale * tail_decay * jnp.einsum('bshq,bhpq->bshp', value_wide, back_in, precision=highest)
    value_grad = jnp.einsum('bhts,bthq->bshq', attn_probs.astype(jnp.float32), grad_wide)
    value_grad = value_grad + score_scale * tail_decay * jnp.einsum('bshp,bhpq->bshq', key_wide, back_in, precision=highest)
    return (new_state, (attention, key_grad, value_grad))

def expert_rows(inputs):
    row_block, weight_in, weight_out = inputs
    slice_width = FF // N_DP
    summed = jnp.zeros((row_block.shape[0], D), jnp.float32)
    for part_index in range(N_DP):
        first_unit = part_index * slice_width
        hidden = jax.nn.silu(lax.dot_general(row_block, weight_in[first_unit:first_unit + slice_width], (((1,), (1,)), ((), ())), preferred_element_type=jnp.float32)).astype(jnp.bfloat16)
        slice_out = jnp.dot(hidden, weight_out[first_unit:first_unit + slice_width], preferred_element_type=jnp.float32).astype(jnp.bfloat16)
        summed = summed + lax.optimization_barrier(slice_out).astype(jnp.float32)
    return summed.astype(jnp.bfloat16)

def reference(queries, keys, values, log_decay, attn_grad, norm_gain, route_ids, route_weights, grad_exponent, w_in, w_out):
    query_blocks = split_heads(queries)
    key_blocks = split_heads(keys)
    value_blocks = split_heads(values)
    grad_blocks = split_heads(attn_grad)
    decay_blocks = split_decay(log_decay)
    zero_state = jnp.zeros((BATCH_SEQUENCES, ATTENTION_HEADS, HEAD, HEAD), jnp.float32)
    unused, back_states = lax.scan(reverse_step, zero_state, (query_blocks, grad_blocks, decay_blocks), reverse=True)
    unused, outputs = lax.scan(forward_step, zero_state, (query_blocks, key_blocks, value_blocks, grad_blocks, decay_blocks, back_states))
    attention, key_grad, value_grad = outputs
    factor = jnp.exp2(grad_exponent.astype(jnp.float32))[:, None]
    attn_out = join_blocks(attention).reshape(BATCH_SEQUENCES, SEQUENCE_LENGTH, D).astype(jnp.bfloat16)
    key_out = (join_blocks(key_grad) * factor).reshape(BATCH_SEQUENCES, SEQUENCE_LENGTH, D).astype(jnp.bfloat16)
    value_out = (join_blocks(value_grad) * factor).reshape(BATCH_SEQUENCES, SEQUENCE_LENGTH, D).astype(jnp.bfloat16)
    attn_wide = attn_out.reshape(BATCH_SEQUENCES * SEQUENCE_LENGTH, D).astype(jnp.float32)
    mean_square = lax.optimization_barrier(jnp.mean(attn_wide * attn_wide, axis=-1, keepdims=True))
    normed = (attn_wide * lax.rsqrt(mean_square + norm_eps) * norm_gain).astype(jnp.bfloat16)
    blocks_count = BATCH_SEQUENCES * N_SEQ
    choice_ids = route_ids.reshape(blocks_count, TOK_DEV * TOP).astype(jnp.int32)
    onehot = (choice_ids[..., None] == jnp.arange(EXPERTS, dtype=jnp.int32)[None, None, :]).astype(jnp.int32)
    counted = jnp.cumsum(onehot, axis=1).astype(jnp.int32)
    slot_index = lax.optimization_barrier(jnp.sum((counted - 1) * onehot, axis=-1)).astype(jnp.int32)
    block_index = jnp.arange(blocks_count, dtype=jnp.int32)[:, None]
    target = ((choice_ids * blocks_count + block_index) * CAP + slot_index).reshape(-1).astype(jnp.int32)
    token_rows = jnp.repeat(normed, TOP, axis=0)
    buffer_rows = jnp.zeros((EXPERTS * blocks_count * CAP, D), jnp.bfloat16).at[target].set(token_rows)
    expert_out = lax.map(expert_rows, (buffer_rows.reshape(EXPERTS, blocks_count * CAP, D), w_in, w_out))
    picked = expert_out.reshape(EXPERTS * blocks_count * CAP, D)[target].reshape(BATCH_SEQUENCES * SEQUENCE_LENGTH, TOP, D)
    mixed_rows = attn_wide + lax.optimization_barrier(jnp.sum(route_weights.reshape(BATCH_SEQUENCES * SEQUENCE_LENGTH, TOP)[..., None] * picked.astype(jnp.float32), axis=1))
    layer_out = mixed_rows.astype(jnp.bfloat16).reshape(BATCH_SEQUENCES, SEQUENCE_LENGTH, D)
    return (layer_out, key_out, value_out)
```

```python
import functools
import jax
import jax.numpy as jnp
from jax import lax
from jax.experimental import pallas as pl
from jax.experimental.pallas import tpu as pltpu
from jax.sharding import PartitionSpec as P

MESH = pl.DeviceIdType.MESH
BF = jnp.bfloat16
F32 = jnp.float32
HOP = 13


def greet(ndp, nseq, dp, me):
    barrier = pltpu.get_barrier_semaphore()

    def plane(d, carry):
        pl.semaphore_signal(
            barrier, inc=1, device_id=(dp, lax.rem(me + HOP * d, nseq)), device_id_type=MESH
        )
        return carry

    for j in range(1, ndp):
        pl.semaphore_signal(
            barrier, inc=1, device_id=(lax.rem(dp + j, ndp), me), device_id_type=MESH
        )
    lax.fori_loop(1, nseq, plane, 0)
    pl.semaphore_wait(barrier, nseq - 1 + ndp - 1)


def push(src, dst, send, recv, z, e):
    pltpu.make_async_remote_copy(
        src_ref=src, dst_ref=dst, send_sem=send, recv_sem=recv, device_id=(z, e), device_id_type=MESH
    ).start()


def landed(ref, sem):
    pltpu.make_async_copy(ref, ref, sem).wait()


def interleave(n_first, n_second, first, second):
    both = min(n_first, n_second)

    def pair(i, carry):
        first(i)
        second(i)
        return carry

    def rest(i, carry):
        (first if n_first > n_second else second)(i)
        return carry

    lax.fori_loop(0, both, pair, 0)
    lax.fori_loop(both, max(n_first, n_second), rest, 0)


def each(n, body):
    def step(i, carry):
        body(i)
        return carry

    lax.fori_loop(0, n, step, 0)


def vmem(*shape, kind=BF):
    return pltpu.VMEM(shape, kind)


HEADS_AT_ONCE = 4


def ramp(run, h):
    size = run.shape[1]
    across = jnp.broadcast_to(run[pl.ds(h, 1), :], (size, size))
    down = jnp.transpose(across)
    return across, down


def lower(size):
    return lax.broadcasted_iota(jnp.int32, (size, size), 0) >= lax.broadcasted_iota(
        jnp.int32, (size, size), 1
    )


def head_span(h, head):
    return pl.ds(pl.multiple_of(h * head, head), head)


def outer(a, b):
    return lax.dot_general(a, b, (((0,), (0,)), ((), ())), preferred_element_type=F32)


def inner(a, b):
    return lax.dot_general(a, b, (((1,), (1,)), ((), ())), preferred_element_type=F32)


def attention_kernel(
    cfg, q, k, v, g, run, gain, attn_out, normed, back, core, fsend, frecv, fout, fin, bsend, brecv,
    fs, fr, gs, gr, bs, br,
):
    ndp, nseq, head = cfg
    tokens = q.shape[0]
    scale = 1.0 / head
    dp = lax.axis_index("dp")
    me = lax.axis_index("seq")
    greet(1, nseq, dp, me)

    def heads(body):
        def group(i, carry):
            for u in range(HEADS_AT_ONCE):
                body(lax.rem(me + HOP * (i * HEADS_AT_ONCE + u), nseq))
            return carry

        lax.fori_loop(0, nseq // HEADS_AT_ONCE, group, 0)

    def forward_local(h):
        cols = head_span(h, head)
        across, down = ramp(run, h)
        total = across[0:1, tokens - 1 : tokens]
        tail = jnp.exp(total - down)
        lifted = (k[:, cols].astype(F32) * tail).astype(BF)
        fsend[h, pl.ds(0, head)] = outer(lifted, v[:, cols]).astype(BF)
        decay = jnp.broadcast_to(jnp.exp(total), (8, head))
        high = decay.astype(BF)
        fsend[h, pl.ds(head, 8)] = high
        fsend[h, pl.ds(head + 8, 8)] = (decay - high.astype(F32)).astype(BF)

        @pl.when(h != me)
        def _():
            push(fsend.at[h], frecv.at[me], fs, fr, dp, h)

    heads(forward_local)
    frecv[me] = fsend[me]
    mask = lower(tokens)

    def inside(h):
        cols = head_span(h, head)
        across, down = ramp(run, h)
        weight = jnp.where(mask, jnp.exp(jnp.where(mask, down - across, 0.0)), 0.0)
        probs = (inner(q[:, cols], k[:, cols]) * weight * scale).astype(BF)
        core[:, cols] = jnp.dot(probs, v[:, cols], preferred_element_type=F32)

    heads(inside)

    def backward_local(h):
        cols = head_span(h, head)
        across, down = ramp(run, h)
        lifted = (q[:, cols].astype(F32) * jnp.exp(down)).astype(BF)
        bsend[h] = outer(lifted, g[:, cols]).astype(BF)

    heads(backward_local)
    landed(frecv.at[pl.ds(0, nseq - 1)], fr)

    def decay_of(i):
        pair = frecv[i, pl.ds(head, 16)].astype(F32)
        return pair[0:1] + pair[8:9]

    def forward_scan(i, state):
        fout[i] = state.astype(BF)

        @pl.when(i != me)
        def _():
            push(fout.at[i], fin.at[me], gs, gr, dp, i)

        return decay_of(i) * state + frecv[i, pl.ds(0, head)].astype(F32)

    lax.fori_loop(0, nseq, forward_scan, jnp.zeros((head, head), F32))
    fin[me] = fout[me]

    def backward_push(d, carry):
        h = lax.rem(me + HOP * d, nseq)
        push(bsend.at[h], brecv.at[me], bs, br, dp, h)
        return carry

    lax.fori_loop(1, nseq, backward_push, 0)
    brecv[me] = bsend[me]
    landed(fin.at[pl.ds(0, nseq - 1)], gr)

    def join(i, square):
        for u in range(HEADS_AT_ONCE):
            h = i * HEADS_AT_ONCE + u
            cols = head_span(h, head)
            across, down = ramp(run, h)
            far = jnp.dot(q[:, cols], fin[h], preferred_element_type=F32)
            total = (core[:, cols] + scale * jnp.exp(down) * far).astype(BF)
            attn_out[:, cols] = total
            wide = total.astype(F32)
            square = square + wide * wide
        return square

    square = lax.fori_loop(0, nseq // HEADS_AT_ONCE, join, jnp.zeros((tokens, head), F32))
    mean = jnp.sum(square, axis=1, keepdims=True) * (1.0 / q.shape[1])
    factor = lax.rsqrt(mean + norm_eps)

    def norm(h):
        cols = head_span(h, head)
        normed[:, cols] = (attn_out[:, cols].astype(F32) * factor * gain[:, cols]).astype(BF)

    each(nseq, norm)
    landed(brecv.at[pl.ds(0, nseq - 1)], br)

    def backward_scan(j, state):
        i = nseq - 1 - j
        back[i] = state.astype(BF)
        return decay_of(i) * state + brecv[i].astype(F32)

    lax.fori_loop(0, nseq, backward_scan, jnp.zeros((head, head), F32))
    landed(fsend.at[pl.ds(0, nseq - 1)], fs)
    landed(fout.at[pl.ds(0, nseq - 1)], gs)
    landed(bsend.at[pl.ds(0, nseq - 1)], bs)


def gradients(head, q, k, v, g, run, factor, back_in, key_out, value_out, count):
    tokens = q.shape[0]
    scale = 1.0 / head
    mask = lower(tokens)

    def group(i, carry):
        for u in range(HEADS_AT_ONCE):
            h = i * HEADS_AT_ONCE + u
            cols = head_span(h, head)
            across, down = ramp(run, h)
            tail = jnp.exp(across[0:1, tokens - 1 : tokens] - down) * scale
            weight = jnp.where(mask, jnp.exp(jnp.where(mask, down - across, 0.0)), 0.0)
            qh, kh, vh, gh = q[:, cols], k[:, cols], v[:, cols], g[:, cols]
            state = back_in[h]
            power = factor[pl.ds(h, 1), :]
            probs = (inner(qh, kh) * weight * scale).astype(BF)
            pulled = (inner(gh, vh) * weight * scale).astype(BF)
            key_grad = outer(pulled, qh) + tail * inner(vh, state)
            value_grad = outer(probs, gh) + tail * jnp.dot(kh, state, preferred_element_type=F32)
            key_out[:, cols] = (key_grad * power).astype(BF)
            value_out[:, cols] = (value_grad * power).astype(BF)
        return carry

    lax.fori_loop(0, count // HEADS_AT_ONCE, group, 0)


def attention(q, k, v, g, run, gain, ndp, nseq, head):
    tokens, model = q.shape
    dma = pltpu.SemaphoreType.DMA
    whole = pl.BlockSpec(memory_space=pltpu.VMEM)
    return pl.pallas_call(
        functools.partial(attention_kernel, (ndp, nseq, head)),
        out_shape=(
            jax.ShapeDtypeStruct((tokens, model), BF),
            jax.ShapeDtypeStruct((tokens, model), BF),
            jax.ShapeDtypeStruct((nseq, head, head), BF),
        ),
        in_specs=[whole] * 6,
        out_specs=(whole,) * 3,
        scratch_shapes=[
            vmem(tokens, model, kind=F32),
            vmem(nseq, head + 16, head),
            vmem(nseq, head + 16, head),
            vmem(nseq, head, head),
            vmem(nseq, head, head),
            vmem(nseq, head, head),
            vmem(nseq, head, head),
            dma, dma, dma, dma, dma, dma,
        ],
        compiler_params=pltpu.CompilerParams(
            collective_id=0, has_side_effects=True, vmem_limit_bytes=40 << 20
        ),
        name="attention",
    )(q, k, v, g, run, gain)


def dispatch_kernel(
    cfg, normed, meta, w_in, q, k, v, g, run, factor, back, hid, meta_all, key_out, value_out,
    x, send_a, send_b, tok, mets, onehot, wv, acc, back_in,
    wsem, ms, mr, ts, tr, as_, ar, bs, br, fs, fr, gs, gr,
):
    ndp, nseq, cap, width, n_a, n_b = cfg
    head = back.shape[1]
    ca = n_a * width
    rows = nseq * cap
    dp = lax.axis_index("dp")
    me = lax.axis_index("seq")
    near = (1, ndp - 1) + tuple(range(2, ndp - 1))

    def span(i, start=0):
        return pl.ds(pl.multiple_of(start + i * width, width), width)

    load_w = pltpu.make_async_copy(w_in.at[0], wv, wsem)
    load_w.start()
    greet(ndp, nseq, dp, me)
    for j in range(1, ndp):
        push(meta, mets.at[dp], ms, mr, lax.rem(dp + j, ndp), me)

    def give(c):
        for j in near:
            z = lax.rem(dp + j, ndp)
            push(normed.at[:, span(c, ca)], tok.at[dp, :, span(c)], ts, tr.at[c], z, me)

    each(n_b, give)

    def spread(d, carry):
        i = lax.rem(me + HOP * d, nseq)
        push(back.at[i], back_in.at[me], gs, gr, dp, i)
        return carry

    lax.fori_loop(1, nseq, spread, 0)
    back_in[me] = back[me]
    mets[dp] = meta[...]

    def select(z):
        slots = lax.broadcasted_iota(jnp.int32, (rows, meta.shape[1]), 0).astype(F32)
        m = mets[z]
        hit = (slots == m[0:1]) | (slots == m[1:2])
        onehot[z] = jnp.where(hit, 1.0, 0.0).astype(BF)

    select(dp)

    def plane_a(a):
        cols = span(a)
        part = jnp.dot(onehot[dp], normed[:, cols], preferred_element_type=F32).astype(BF)
        send_a[:, :, :, cols] = part.reshape(nseq, cap // 2, 2, width)
        x[dp, me, :, :, cols] = send_a[me, :, :, cols]

        def go(d, carry):
            e = lax.rem(me + HOP * d, nseq)
            push(send_a.at[e, :, :, cols], x.at[dp, me, :, :, cols], as_, ar.at[a], dp, e)
            return carry

        lax.fori_loop(1, nseq, go, 0)

    each(n_a, plane_a)

    def own(c):
        tok[dp, :, span(c)] = normed[:, span(c, ca)]

    each(n_b, own)
    landed(mets.at[pl.ds(0, ndp - 1)], mr)
    for j in range(1, ndp):
        select(lax.rem(dp + j, ndp))

    def plane_b(i):
        cols, there = span(i), span(i, ca)
        landed(tok.at[pl.ds(0, ndp - 1), :, cols], tr.at[i])

        def build(z):
            part = jnp.dot(onehot[z], tok[z, :, cols], preferred_element_type=F32).astype(BF)
            send_b[z, :, :, :, cols] = part.reshape(nseq, cap // 2, 2, width)
            x[z, me, :, :, there] = send_b[z, me, :, :, cols]

        each(ndp, build)

        def go(d, carry):
            e = lax.rem(me + HOP * d, nseq)
            push(send_b.at[:, e, :, :, cols], x.at[:, me, :, :, there], bs, br.at[i], dp, e)
            return carry

        lax.fori_loop(1, nseq, go, 0)

    def onward_a(i):
        cols = span(i)
        landed(x.at[dp, pl.ds(0, nseq - 1), :, :, cols], ar.at[i])
        for j in near:
            z = lax.rem(dp + j, ndp)
            push(x.at[dp, :, :, :, cols], x.at[dp, :, :, :, cols], fs, fr.at[i], z, me)

    interleave(n_b, n_a, plane_b, onward_a)

    landed(back_in.at[pl.ds(0, nseq - 1)], gr)
    gradients(head, q, k, v, g, run, factor, back_in, key_out, value_out, nseq)

    def clear(z):
        here = pl.ds(pl.multiple_of(z * rows, rows), rows)
        acc[here] = jnp.zeros((rows, acc.shape[1]), F32)

    each(ndp, clear)
    load_w.wait()

    def absorb(cols):
        def part(z):
            block = x[z, :, :, :, cols].reshape(rows, width)
            here = pl.ds(pl.multiple_of(z * rows, rows), rows)
            acc[here] += lax.dot_general(
                block, wv[:, cols], (((1,), (1,)), ((), ())), preferred_element_type=F32
            )

        each(ndp, part)

    def absorb_b(i):
        cols = span(i, ca)
        landed(x.at[:, pl.ds(0, nseq - 1), :, :, cols], br.at[i])
        absorb(cols)

    def absorb_a(i):
        cols = span(i)
        landed(x.at[pl.ds(0, ndp - 1), :, :, :, cols], fr.at[i])
        absorb(cols)

    interleave(n_b, n_a, absorb_b, absorb_a)

    def finish(z):
        here = pl.ds(pl.multiple_of(z * rows, rows), rows)
        hid[here] = jax.nn.silu(acc[here]).astype(BF)

    each(ndp, finish)
    meta_all[...] = mets[...]
    landed(back.at[pl.ds(0, nseq - 1)], gs)
    landed(mets.at[pl.ds(0, ndp - 1)], ms)
    if n_b:
        landed(tok.at[pl.ds(0, ndp - 1)], ts)
        landed(send_b.at[:, pl.ds(0, nseq - 1)], bs)
    if n_a:
        landed(send_a.at[pl.ds(0, nseq - 1)], as_)
        landed(x.at[pl.ds(0, ndp - 1), :, :, :, pl.ds(0, ca)], fs)


def combine_kernel(
    cfg, hid, meta_all, w_out, base, out, own_a, part_b, from_z, send_a, ret_a, ret_b, sums, got, mix, wv,
    wsem, zs, zr, bs, br, as_, ar, ss, sr,
):
    ndp, nseq, cap, width, n_a, n_b = cfg
    ca = n_a * width
    rows = nseq * cap
    tokens = base.shape[0]
    dp = lax.axis_index("dp")
    me = lax.axis_index("seq")
    near = (1, ndp - 1) + tuple(range(2, ndp - 1))

    def span(i, start=0):
        return pl.ds(pl.multiple_of(start + i * width, width), width)

    def fetch(cols, c):
        return pltpu.make_async_copy(w_out.at[0, :, cols], wv.at[:, cols], wsem.at[c])

    interleave(
        n_b, n_a,
        lambda i: fetch(span(i, ca), n_a + i).start(),
        lambda i: fetch(span(i), i).start(),
    )
    greet(ndp, nseq, dp, me)

    def second(z, cols):
        here = pl.ds(pl.multiple_of(z * rows, rows), rows)
        y = jnp.dot(hid[here], wv[:, cols], preferred_element_type=F32)
        return y.astype(BF).reshape(nseq, cap // 2, 2, width)

    def make_b(i):
        cols, there = span(i), span(i, ca)
        fetch(there, n_a + i).wait()

        def part(z):
            part_b[z, :, :, :, cols] = second(z, there)
            ret_b[z, me, :, :, cols] = part_b[z, me, :, :, cols]

        each(ndp, part)

        def go(d, carry):
            e = lax.rem(me + HOP * d, nseq)
            push(part_b.at[:, e, :, :, cols], ret_b.at[:, me, :, :, cols], bs, br.at[i], dp, e)
            return carry

        lax.fori_loop(1, nseq, go, 0)

    def make_a(i):
        cols = span(i)
        fetch(cols, i).wait()

        def part(z):
            own_a[z, :, :, :, cols] = second(z, cols)

        each(ndp, part)
        for j in near:
            z = lax.rem(dp + j, ndp)
            push(own_a.at[z, :, :, :, cols], from_z.at[dp, :, :, :, cols], zs, zr.at[i], z, me)

    interleave(n_b, n_a, make_b, make_a)

    eye = jnp.where(
        lax.broadcasted_iota(jnp.int32, (tokens, tokens), 0)
        == lax.broadcasted_iota(jnp.int32, (tokens, tokens), 1), 1.0, 0.0,
    ).astype(BF)

    def weigh(z):
        slots = lax.broadcasted_iota(jnp.int32, (rows, tokens), 0).astype(F32)
        m = meta_all[z]
        pick = jnp.where(slots == m[0:1], m[2:3], 0.0) + jnp.where(slots == m[1:2], m[3:4], 0.0)
        mix[z] = lax.dot_general(
            eye, pick.astype(BF), (((1,), (1,)), ((), ())), preferred_element_type=F32
        ).astype(BF)

    each(ndp, weigh)

    def back_a(i):
        cols = span(i)
        landed(from_z.at[pl.ds(0, ndp - 1), :, :, :, cols], zr.at[i])

        def add(e, carry):
            some = pl.ds(e * 4, 4)
            flat = (4 * cap, width)
            total = own_a[dp, some, :, :, cols].reshape(flat).astype(F32)
            for j in range(1, ndp):
                z = lax.rem(dp + j, ndp)
                total = total + from_z[z, some, :, :, cols].reshape(flat).astype(F32)
            send_a[some, :, :, cols] = total.astype(BF).reshape(4, cap // 2, 2, width)
            return carry

        lax.fori_loop(0, nseq // 4, add, 0)
        ret_a[me, :, :, cols] = send_a[me, :, :, cols]

        def go(d, carry):
            e = lax.rem(me + HOP * d, nseq)
            push(send_a.at[e, :, :, cols], ret_a.at[me, :, :, cols], as_, ar.at[i], dp, e)
            return carry

        lax.fori_loop(1, nseq, go, 0)

    def mix_b(i):
        cols = span(i)
        landed(ret_b.at[:, pl.ds(0, nseq - 1), :, :, cols], br.at[i])

        def part(z):
            block = ret_b[z, :, :, :, cols].reshape(rows, width)
            sums[z, :, cols] = jnp.dot(mix[z], block, preferred_element_type=F32).astype(BF)

        each(ndp, part)
        for j in near:
            z = lax.rem(dp + j, ndp)
            push(sums.at[z, :, cols], got.at[dp, :, cols], ss, sr.at[i], z, me)

    interleave(n_b, n_a, mix_b, back_a)

    def end_a(i):
        cols = span(i)
        landed(ret_a.at[pl.ds(0, nseq - 1), :, :, cols], ar.at[i])
        block = ret_a[:, :, :, cols].reshape(rows, width)
        mixed = jnp.dot(mix[dp], block, preferred_element_type=F32)
        out[:, cols] = (base[:, cols].astype(F32) + mixed).astype(BF)

    def end_b(i):
        cols, there = span(i), span(i, ca)
        landed(got.at[pl.ds(0, ndp - 1), :, cols], sr.at[i])
        total = sums[dp, :, cols].astype(F32)
        for j in range(1, ndp):
            total = total + got[lax.rem(dp + j, ndp), :, cols].astype(F32)
        out[:, there] = (base[:, there].astype(F32) + total).astype(BF)

    interleave(n_b, n_a, end_b, end_a)
    if n_a:
        landed(own_a.at[pl.ds(0, ndp - 1)], zs)
        landed(send_a.at[pl.ds(0, nseq - 1)], as_)
    if n_b:
        landed(part_b.at[:, pl.ds(0, nseq - 1)], bs)
        landed(sums.at[pl.ds(0, ndp - 1)], ss)


def experts(
    normed, base, q, k, v, g, run, factor, back, choice, slot, weights, w_in, w_out, ndp, nseq, cap, split
):
    tokens, model = normed.shape
    hidden = w_in.shape[1]
    n_a, n_b, width = split
    rows = nseq * cap
    ca, cb = n_a * width, n_b * width
    cfg = (ndp, nseq, cap, width, n_a, n_b)
    target = (choice * cap + slot).astype(F32).T
    meta = jnp.concatenate([target, weights.T, jnp.zeros((4, tokens), F32)], axis=0)
    dma = pltpu.SemaphoreType.DMA
    whole = pl.BlockSpec(memory_space=pltpu.VMEM)
    away = pl.BlockSpec(memory_space=pl.ANY)
    hid, meta_all, key_out, value_out = pl.pallas_call(
        functools.partial(dispatch_kernel, cfg),
        out_shape=(
            jax.ShapeDtypeStruct((ndp * rows, hidden), BF),
            jax.ShapeDtypeStruct((ndp, 8, tokens), F32),
            jax.ShapeDtypeStruct((tokens, model), BF),
            jax.ShapeDtypeStruct((tokens, model), BF),
        ),
        in_specs=[whole, whole, away] + [whole] * 7,
        out_specs=(whole,) * 4,
        scratch_shapes=[
            vmem(ndp, nseq, cap // 2, 2, model),
            vmem(nseq, cap // 2, 2, max(ca, 128)),
            vmem(ndp, nseq, cap // 2, 2, max(cb, 128)),
            vmem(ndp, tokens, max(cb, 128)),
            vmem(ndp, 8, tokens, kind=F32),
            vmem(ndp, rows, tokens),
            vmem(hidden, model),
            vmem(ndp * rows, hidden, kind=F32),
            vmem(*back.shape),
            dma, dma, dma, dma, dma((max(n_b, 1),)), dma, dma((max(n_a, 1),)),
            dma, dma((max(n_b, 1),)), dma, dma((max(n_a, 1),)), dma, dma,
        ],
        compiler_params=pltpu.CompilerParams(
            collective_id=1, has_side_effects=True, vmem_limit_bytes=62 << 20
        ),
        name="dispatch",
    )(normed, meta, w_in, q, k, v, g, run, factor, back)
    layer_out = pl.pallas_call(
        functools.partial(combine_kernel, cfg),
        out_shape=jax.ShapeDtypeStruct((tokens, model), BF),
        in_specs=[whole, whole, away, whole],
        out_specs=whole,
        scratch_shapes=[
            vmem(ndp, nseq, cap // 2, 2, max(ca, 128)),
            vmem(ndp, nseq, cap // 2, 2, max(cb, 128)),
            vmem(ndp, nseq, cap // 2, 2, max(ca, 128)),
            vmem(nseq, cap // 2, 2, max(ca, 128)),
            vmem(nseq, cap // 2, 2, max(ca, 128)),
            vmem(ndp, nseq, cap // 2, 2, max(cb, 128)),
            vmem(ndp, tokens, max(cb, 128)),
            vmem(ndp, tokens, max(cb, 128)),
            vmem(ndp, tokens, rows),
            vmem(hidden, model),
            dma((n_a + n_b,)), dma, dma((max(n_a, 1),)), dma, dma((max(n_b, 1),)),
            dma, dma((max(n_a, 1),)), dma, dma((max(n_b, 1),)),
        ],
        compiler_params=pltpu.CompilerParams(
            collective_id=2, has_side_effects=True, vmem_limit_bytes=62 << 20
        ),
        name="combine",
    )(hid, meta_all, w_out, base)
    return layer_out, key_out, value_out


norm_eps = 1e-06
TOP = 2
SPLIT = (4, 4, 512)


def on_device(
    queries, keys, values, log_decay, attn_grad, norm_gain, route_ids, route_weights, grad_exponent,
    w_in, w_out,
):
    length, width = queries.shape[1:]
    ndp, nseq = lax.axis_size("dp"), lax.axis_size("seq")
    heads = log_decay.shape[1]
    head = width // heads
    cap = max(2, TOP * length * 5 // (4 * nseq))
    run = jnp.cumsum(log_decay[0], axis=1)
    factor = jnp.broadcast_to(jnp.exp2(grad_exponent.astype(F32))[:, None], (heads, head))
    choice = route_ids[0]
    flat = choice.reshape(length * TOP)
    onehot = (flat[:, None] == jnp.arange(nseq, dtype=jnp.int32)[None, :]).astype(jnp.int32)
    slot = jnp.sum((jnp.cumsum(onehot, axis=0) - 1) * onehot, axis=-1).reshape(length, TOP)
    q, k, v, g = queries[0], keys[0], values[0], attn_grad[0]
    attn_out, normed, back = attention(q, k, v, g, run, norm_gain[None], ndp, nseq, head)
    layer_out, key_out, value_out = experts(
        normed, attn_out, q, k, v, g, run, factor, back, choice, slot, route_weights[0], w_in, w_out,
        ndp, nseq, cap, SPLIT,
    )
    return (layer_out[None], key_out[None], value_out[None])


def solution(mesh):
    rows = P("dp", "seq", None)
    placed = (
        rows, rows, rows, P("dp", None, "seq"), rows, P(), rows, rows, P(),
        P("seq", "dp", None), P("seq", "dp", None),
    )
    return jax.shard_map(
        on_device, mesh=mesh, in_specs=placed, out_specs=(rows, rows, rows), check_vma=False
    )
```

```python
import functools
import jax
import jax.numpy as jnp
from jax import lax
from jax.experimental import pallas as pl
from jax.experimental.pallas import tpu as pltpu
from jax.sharding import PartitionSpec as P

MESH = pl.DeviceIdType.MESH
BF = jnp.bfloat16
F32 = jnp.float32
HOP = 13


def greet(ndp, nseq, dp, me):
    barrier = pltpu.get_barrier_semaphore()

    def plane(d, carry):
        pl.semaphore_signal(
            barrier, inc=1, device_id=(dp, lax.rem(me + HOP * d, nseq)), device_id_type=MESH
        )
        return carry

    for j in range(1, ndp):
        pl.semaphore_signal(
            barrier, inc=1, device_id=(lax.rem(dp + j, ndp), me), device_id_type=MESH
        )
    lax.fori_loop(1, nseq, plane, 0)
    pl.semaphore_wait(barrier, nseq - 1 + ndp - 1)


def push(src, dst, send, recv, z, e):
    pltpu.make_async_remote_copy(
        src_ref=src, dst_ref=dst, send_sem=send, recv_sem=recv, device_id=(z, e), device_id_type=MESH
    ).start()


def landed(ref, sem):
    pltpu.make_async_copy(ref, ref, sem).wait()


def interleave(n_first, n_second, first, second):
    both = min(n_first, n_second)

    def pair(i, carry):
        first(i)
        second(i)
        return carry

    def rest(i, carry):
        (first if n_first > n_second else second)(i)
        return carry

    lax.fori_loop(0, both, pair, 0)
    lax.fori_loop(both, max(n_first, n_second), rest, 0)


def each(n, body):
    def step(i, carry):
        body(i)
        return carry

    lax.fori_loop(0, n, step, 0)


def vmem(*shape, kind=BF):
    return pltpu.VMEM(shape, kind)


HEADS_AT_ONCE = 4


def ramp(run, h):
    size = run.shape[1]
    across = jnp.broadcast_to(run[pl.ds(h, 1), :], (size, size))
    down = jnp.transpose(across)
    return across, down


def lower(size):
    return lax.broadcasted_iota(jnp.int32, (size, size), 0) >= lax.broadcasted_iota(
        jnp.int32, (size, size), 1
    )


def head_span(h, head):
    return pl.ds(pl.multiple_of(h * head, head), head)


def outer(a, b):
    return lax.dot_general(a, b, (((0,), (0,)), ((), ())), preferred_element_type=F32)


def inner(a, b):
    return lax.dot_general(a, b, (((1,), (1,)), ((), ())), preferred_element_type=F32)


def attention_kernel(
    cfg, q_far, k_far, v_far, g_far, decay, gain, ids, weights, attn_out, normed, back, run, meta,
    q, k, v, g, core, fsend, frecv, fout, fin, bsend, brecv, ls, fs, fr, gs, gr, bs, br,
):
    ndp, nseq, head, cap = cfg
    tokens = q.shape[0]
    scale = 1.0 / head
    dp = lax.axis_index("dp")
    me = lax.axis_index("seq")
    loads = [
        pltpu.make_async_copy(far.at[0], near, ls.at[n])
        for n, (far, near) in enumerate(((k_far, k), (v_far, v), (q_far, q), (g_far, g)))
    ]
    for load in loads:
        load.start()
    sums = decay[0]
    lane = lax.broadcasted_iota(jnp.int32, sums.shape, 1)
    step = 1
    while step < tokens:
        sums = sums + jnp.where(lane >= step, pltpu.roll(sums, step, 1), 0.0)
        step *= 2
    run[...] = sums
    greet(1, nseq, dp, me)
    loads[0].wait()
    loads[1].wait()

    def heads(body):
        def group(i, carry):
            for u in range(HEADS_AT_ONCE):
                body(lax.rem(me + HOP * (i * HEADS_AT_ONCE + u), nseq))
            return carry

        lax.fori_loop(0, nseq // HEADS_AT_ONCE, group, 0)

    def forward_local(h):
        cols = head_span(h, head)
        across, down = ramp(run, h)
        total = across[0:1, tokens - 1 : tokens]
        tail = jnp.exp(total - down)
        lifted = (k[:, cols].astype(F32) * tail).astype(BF)
        fsend[h, pl.ds(0, head)] = outer(lifted, v[:, cols]).astype(BF)
        decay = jnp.broadcast_to(jnp.exp(total), (8, head))
        high = decay.astype(BF)
        fsend[h, pl.ds(head, 8)] = high
        fsend[h, pl.ds(head + 8, 8)] = (decay - high.astype(F32)).astype(BF)

        @pl.when(h != me)
        def _():
            push(fsend.at[h], frecv.at[me], fs, fr, dp, h)

    heads(forward_local)
    frecv[me] = fsend[me]
    mask = lower(tokens)
    first, second = ids[0, 0:1], ids[0, 1:2]
    owner = lax.broadcasted_iota(jnp.int32, (nseq, tokens), 0)
    named = ((owner == first) | (owner == second)).astype(F32).astype(BF)
    before = jnp.where(mask, 0.0, 1.0).astype(BF)
    slots = jnp.dot(named, before, preferred_element_type=F32) + (owner * cap).astype(F32)
    for row, choice in enumerate((first, second)):
        meta[row : row + 1] = jnp.sum(jnp.where(owner == choice, slots, 0.0), axis=0, keepdims=True)
    meta[2:4] = weights[0]
    meta[4:8] = jnp.zeros((4, tokens), F32)
    loads[2].wait()
    loads[3].wait()

    def inside(h):
        cols = head_span(h, head)
        across, down = ramp(run, h)
        weight = jnp.where(mask, jnp.exp(jnp.where(mask, down - across, 0.0)), 0.0)
        probs = (inner(q[:, cols], k[:, cols]) * weight * scale).astype(BF)
        core[:, cols] = jnp.dot(probs, v[:, cols], preferred_element_type=F32)

    heads(inside)

    def backward_local(h):
        cols = head_span(h, head)
        across, down = ramp(run, h)
        lifted = (q[:, cols].astype(F32) * jnp.exp(down)).astype(BF)
        bsend[h] = outer(lifted, g[:, cols]).astype(BF)

    heads(backward_local)
    landed(frecv.at[pl.ds(0, nseq - 1)], fr)

    def decay_of(i):
        pair = frecv[i, pl.ds(head, 16)].astype(F32)
        return pair[0:1] + pair[8:9]

    def forward_scan(i, state):
        fout[i] = state.astype(BF)

        @pl.when(i != me)
        def _():
            push(fout.at[i], fin.at[me], gs, gr, dp, i)

        return decay_of(i) * state + frecv[i, pl.ds(0, head)].astype(F32)

    lax.fori_loop(0, nseq, forward_scan, jnp.zeros((head, head), F32))
    fin[me] = fout[me]

    def backward_push(d, carry):
        h = lax.rem(me + HOP * d, nseq)
        push(bsend.at[h], brecv.at[me], bs, br, dp, h)
        return carry

    lax.fori_loop(1, nseq, backward_push, 0)
    brecv[me] = bsend[me]
    landed(fin.at[pl.ds(0, nseq - 1)], gr)

    def join(i, square):
        for u in range(HEADS_AT_ONCE):
            h = i * HEADS_AT_ONCE + u
            cols = head_span(h, head)
            across, down = ramp(run, h)
            far = jnp.dot(q[:, cols], fin[h], preferred_element_type=F32)
            total = (core[:, cols] + scale * jnp.exp(down) * far).astype(BF)
            attn_out[:, cols] = total
            wide = total.astype(F32)
            square = square + wide * wide
        return square

    square = lax.fori_loop(0, nseq // HEADS_AT_ONCE, join, jnp.zeros((tokens, head), F32))
    mean = jnp.sum(square, axis=1, keepdims=True) * (1.0 / q.shape[1])
    factor = lax.rsqrt(mean + norm_eps)

    def norm(h):
        cols = head_span(h, head)
        normed[:, cols] = (attn_out[:, cols].astype(F32) * factor * gain[:, cols]).astype(BF)

    each(nseq, norm)
    landed(brecv.at[pl.ds(0, nseq - 1)], br)

    def backward_scan(j, state):
        i = nseq - 1 - j
        back[i] = state.astype(BF)
        return decay_of(i) * state + brecv[i].astype(F32)

    lax.fori_loop(0, nseq, backward_scan, jnp.zeros((head, head), F32))
    landed(fsend.at[pl.ds(0, nseq - 1)], fs)
    landed(fout.at[pl.ds(0, nseq - 1)], gs)
    landed(bsend.at[pl.ds(0, nseq - 1)], bs)


def gradients(head, q, k, v, g, run, factor, back_in, key_out, value_out, count):
    tokens = q.shape[0]
    scale = 1.0 / head
    mask = lower(tokens)

    def group(i, carry):
        for u in range(HEADS_AT_ONCE):
            h = i * HEADS_AT_ONCE + u
            cols = head_span(h, head)
            across, down = ramp(run, h)
            tail = jnp.exp(across[0:1, tokens - 1 : tokens] - down) * scale
            weight = jnp.where(mask, jnp.exp(jnp.where(mask, down - across, 0.0)), 0.0)
            qh, kh, vh, gh = q[:, cols], k[:, cols], v[:, cols], g[:, cols]
            state = back_in[h]
            power = factor[pl.ds(h, 1), :]
            probs = (inner(qh, kh) * weight * scale).astype(BF)
            pulled = (inner(gh, vh) * weight * scale).astype(BF)
            key_grad = outer(pulled, qh) + tail * inner(vh, state)
            value_grad = outer(probs, gh) + tail * jnp.dot(kh, state, preferred_element_type=F32)
            key_out[:, cols] = (key_grad * power).astype(BF)
            value_out[:, cols] = (value_grad * power).astype(BF)
        return carry

    lax.fori_loop(0, count // HEADS_AT_ONCE, group, 0)


def attention(q, k, v, g, decay, gain, ids, weights, ndp, nseq, head, cap):
    tokens, model = q.shape[1:]
    dma = pltpu.SemaphoreType.DMA
    whole = pl.BlockSpec(memory_space=pltpu.VMEM)
    away = pl.BlockSpec(memory_space=pl.ANY)
    return pl.pallas_call(
        functools.partial(attention_kernel, (ndp, nseq, head, cap)),
        out_shape=(
            jax.ShapeDtypeStruct((tokens, model), BF),
            jax.ShapeDtypeStruct((tokens, model), BF),
            jax.ShapeDtypeStruct((nseq, head, head), BF),
            jax.ShapeDtypeStruct((nseq, tokens), F32),
            jax.ShapeDtypeStruct((8, tokens), F32),
        ),
        in_specs=[away] * 4 + [whole] * 4,
        out_specs=(whole,) * 5,
        scratch_shapes=[
            vmem(tokens, model),
            vmem(tokens, model),
            vmem(tokens, model),
            vmem(tokens, model),
            vmem(tokens, model, kind=F32),
            vmem(nseq, head + 16, head),
            vmem(nseq, head + 16, head),
            vmem(nseq, head, head),
            vmem(nseq, head, head),
            vmem(nseq, head, head),
            vmem(nseq, head, head),
            dma((4,)), dma, dma, dma, dma, dma, dma,
        ],
        compiler_params=pltpu.CompilerParams(
            collective_id=0, has_side_effects=True, vmem_limit_bytes=62 << 20
        ),
        name="attention",
    )(q, k, v, g, decay, gain, ids, weights)


def dispatch_kernel(
    cfg, normed, meta, w_in, q_far, k_far, v_far, g_far, run, factor, back,
    hid, meta_all, key_out, value_out,
    x, send_a, send_b, tok, mets, onehot, wv, acc, back_in, q, k, v, g,
    wsem, ls, ms, mr, ts, tr, as_, ar, bs, br, fs, fl, fr, hs, hl, hr, gs, gr,
):
    ndp, nseq, cap, width, n_a, n_b = cfg
    head = back.shape[1]
    ca = n_a * width
    rows = nseq * cap
    dp = lax.axis_index("dp")
    me = lax.axis_index("seq")
    near = (1, ndp - 1) + tuple(range(2, ndp - 1))

    def span(i, start=0):
        return pl.ds(pl.multiple_of(start + i * width, width), width)

    load_w = pltpu.make_async_copy(w_in.at[0], wv, wsem)
    loads = [
        pltpu.make_async_copy(far.at[0], close, ls.at[n])
        for n, (far, close) in enumerate(((q_far, q), (k_far, k), (v_far, v), (g_far, g)))
    ]
    load_w.start()
    for load in loads:
        load.start()
    right, left, far_z = lax.rem(dp + 1, ndp), lax.rem(dp + 3, ndp), lax.rem(dp + 2, ndp)
    low, high = pl.ds(0, nseq // 2), pl.ds(nseq // 2, nseq // 2)
    greet(ndp, nseq, dp, me)
    for j in range(1, ndp):
        push(meta, mets.at[dp], ms, mr, lax.rem(dp + j, ndp), me)

    def give(c):
        for j in near:
            z = lax.rem(dp + j, ndp)
            push(normed.at[:, span(c, ca)], tok.at[dp, :, span(c)], ts, tr.at[c], z, me)

    each(n_b, give)

    mets[dp] = meta[...]

    def select(z):
        slots = lax.broadcasted_iota(jnp.int32, (rows, meta.shape[1]), 0).astype(F32)
        m = mets[z]
        hit = (slots == m[0:1]) | (slots == m[1:2])
        onehot[z] = jnp.where(hit, 1.0, 0.0).astype(BF)

    select(dp)

    def plane_a(a):
        cols = span(a)
        part = jnp.dot(onehot[dp], normed[:, cols], preferred_element_type=F32).astype(BF)
        send_a[:, :, :, cols] = part.reshape(nseq, cap // 2, 2, width)
        x[dp, me, :, :, cols] = send_a[me, :, :, cols]

        def go(d, carry):
            e = lax.rem(me + HOP * d, nseq)
            push(send_a.at[e, :, :, cols], x.at[dp, me, :, :, cols], as_, ar.at[a], dp, e)
            return carry

        lax.fori_loop(1, nseq, go, 0)

    each(n_a, plane_a)

    def spread(d, carry):
        i = lax.rem(me + HOP * d, nseq)
        push(back.at[i], back_in.at[me], gs, gr, dp, i)
        return carry

    lax.fori_loop(1, nseq, spread, 0)
    back_in[me] = back[me]

    def own(c):
        tok[dp, :, span(c)] = normed[:, span(c, ca)]

    each(n_b, own)
    landed(mets.at[pl.ds(0, ndp - 1)], mr)
    for j in range(1, ndp):
        select(lax.rem(dp + j, ndp))

    def plane_b(i):
        cols, there = span(i), span(i, ca)
        landed(tok.at[pl.ds(0, ndp - 1), :, cols], tr.at[i])

        def build(z):
            part = jnp.dot(onehot[z], tok[z, :, cols], preferred_element_type=F32).astype(BF)
            send_b[z, :, :, :, cols] = part.reshape(nseq, cap // 2, 2, width)
            x[z, me, :, :, there] = send_b[z, me, :, :, cols]

        each(ndp, build)

        def go(d, carry):
            e = lax.rem(me + HOP * d, nseq)
            push(send_b.at[:, e, :, :, cols], x.at[:, me, :, :, there], bs, br.at[i], dp, e)
            return carry

        lax.fori_loop(1, nseq, go, 0)

    def onward_a(i):
        cols = span(i)
        landed(x.at[dp, pl.ds(0, nseq - 1), :, :, cols], ar.at[i])
        push(x.at[dp, :, :, :, cols], x.at[dp, :, :, :, cols], fs, fl.at[i], right, me)
        push(x.at[dp, :, :, :, cols], x.at[dp, :, :, :, cols], fs, fr.at[i], left, me)

    interleave(n_b, n_a, plane_b, onward_a)

    def clear(z):
        here = pl.ds(pl.multiple_of(z * rows, rows), rows)
        acc[here] = jnp.zeros((rows, acc.shape[1]), F32)

    each(ndp, clear)
    landed(back_in.at[pl.ds(0, nseq - 1)], gr)
    for load in loads:
        load.wait()
    gradients(head, q, k, v, g, run, factor, back_in, key_out, value_out, nseq)
    load_w.wait()

    def absorb(z, cols):
        block = x[z, :, :, :, cols].reshape(rows, width)
        here = pl.ds(pl.multiple_of(z * rows, rows), rows)
        acc[here] += lax.dot_general(
            block, wv[:, cols], (((1,), (1,)), ((), ())), preferred_element_type=F32
        )

    def relay_a(i):
        cols = span(i)
        landed(x.at[left, :, :, :, cols], fl.at[i])
        push(x.at[left, low, :, :, cols], x.at[left, low, :, :, cols], hs, hl.at[i], right, me)
        landed(x.at[right, :, :, :, cols], fr.at[i])
        push(x.at[right, high, :, :, cols], x.at[right, high, :, :, cols], hs, hr.at[i], left, me)

        def part(j):
            absorb(lax.rem(dp + 3 + j, ndp), cols)

        each(3, part)

    each(n_a, relay_a)

    def absorb_b(i):
        cols = span(i, ca)
        landed(x.at[:, pl.ds(0, nseq - 1), :, :, cols], br.at[i])
        each(ndp, lambda z: absorb(z, cols))

    def absorb_a(i):
        cols = span(i)
        landed(x.at[far_z, low, :, :, cols], hl.at[i])
        landed(x.at[far_z, high, :, :, cols], hr.at[i])
        absorb(far_z, cols)

    interleave(n_b, n_a, absorb_b, absorb_a)

    def finish(z):
        here = pl.ds(pl.multiple_of(z * rows, rows), rows)
        hid[here] = jax.nn.silu(acc[here]).astype(BF)

    each(ndp, finish)
    meta_all[...] = mets[...]
    landed(back.at[pl.ds(0, nseq - 1)], gs)
    landed(mets.at[pl.ds(0, ndp - 1)], ms)
    if n_b:
        landed(tok.at[pl.ds(0, ndp - 1)], ts)
        landed(send_b.at[:, pl.ds(0, nseq - 1)], bs)
    if n_a:
        landed(send_a.at[pl.ds(0, nseq - 1)], as_)
        landed(x.at[pl.ds(0, 2), :, :, :, pl.ds(0, ca)], fs)
        landed(x.at[0, :, :, :, pl.ds(0, ca)], hs)


def combine_kernel(
    cfg, hid, meta_all, w_out, base, out, own_a, part_b, half_l, half_r, from_l, from_r, send_a, ret_a, ret_b,
    sums, got, mix, wv, wsem, zs, hl, hr, fs, fl, fr, bs, br, as_, ar, ss, sr,
):
    ndp, nseq, cap, width, n_a, n_b = cfg
    ca = n_a * width
    rows = nseq * cap
    tokens = base.shape[0]
    dp = lax.axis_index("dp")
    me = lax.axis_index("seq")
    near = (1, ndp - 1) + tuple(range(2, ndp - 1))

    def span(i, start=0):
        return pl.ds(pl.multiple_of(start + i * width, width), width)

    def fetch(cols, c):
        return pltpu.make_async_copy(w_out.at[0, :, cols], wv.at[:, cols], wsem.at[c])

    interleave(
        n_a, n_b,
        lambda i: fetch(span(i), i).start(),
        lambda i: fetch(span(i, ca), n_a + i).start(),
    )
    right, left, far_z = lax.rem(dp + 1, ndp), lax.rem(dp + 3, ndp), lax.rem(dp + 2, ndp)
    mid = nseq // 2
    low, high = pl.ds(0, mid), pl.ds(mid, mid)
    greet(ndp, nseq, dp, me)

    def second(z, cols):
        here = pl.ds(pl.multiple_of(z * rows, rows), rows)
        y = jnp.dot(hid[here], wv[:, cols], preferred_element_type=F32)
        return y.astype(BF).reshape(nseq, cap // 2, 2, width)

    def make_b(i):
        cols, there = span(i), span(i, ca)
        fetch(there, n_a + i).wait()

        def part(z):
            part_b[z, :, :, :, cols] = second(z, there)
            ret_b[z, me, :, :, cols] = part_b[z, me, :, :, cols]

        each(ndp, part)

        def go(d, carry):
            e = lax.rem(me + HOP * d, nseq)
            push(part_b.at[:, e, :, :, cols], ret_b.at[:, me, :, :, cols], bs, br.at[i], dp, e)
            return carry

        lax.fori_loop(1, nseq, go, 0)

    def make_a(i):
        cols = span(i)
        fetch(cols, i).wait()

        def part(z):
            own_a[z, :, :, :, cols] = second(z, cols)

        part(far_z)
        push(own_a.at[far_z, low, :, :, cols], half_l.at[:, :, :, cols], zs, hl.at[i], right, me)
        push(own_a.at[far_z, high, :, :, cols], half_r.at[:, :, :, cols], zs, hr.at[i], left, me)
        each(3, lambda j: part(lax.rem(dp + 3 + j, ndp)))

    def join(target, source, z, start, cols, n):
        batch = min(4, n)
        flat = (batch * cap, width)

        def some(e):
            here, there = pl.ds(start + e * batch, batch), pl.ds(e * batch, batch)
            total = target[z, here, :, :, cols].reshape(flat).astype(F32)
            total = total + source[there, :, :, cols].reshape(flat).astype(F32)
            target[z, here, :, :, cols] = total.astype(BF).reshape(batch, cap // 2, 2, width)

        each(n // batch, some)

    def turn_a(i):
        cols = span(i)
        landed(half_l.at[:, :, :, cols], hl.at[i])
        join(own_a, half_l, right, 0, cols, mid)
        push(own_a.at[right, :, :, :, cols], from_l.at[:, :, :, cols], fs, fl.at[i], right, me)
        landed(half_r.at[:, :, :, cols], hr.at[i])
        join(own_a, half_r, left, mid, cols, mid)
        push(own_a.at[left, :, :, :, cols], from_r.at[:, :, :, cols], fs, fr.at[i], left, me)

    both = min(n_a, n_b)

    def make(i):
        make_a(i)
        if_later(i, turn_a)
        make_b(i)

    def if_later(i, body):
        @pl.when(i > 0)
        def _():
            body(i - 1)

    each(both, make)

    def make_more(i, carry):
        if n_a > n_b:
            make_a(i)
            if_later(i, turn_a)
        else:
            make_b(i)
        return carry

    lax.fori_loop(both, max(n_a, n_b), make_more, 0)

    eye = jnp.where(
        lax.broadcasted_iota(jnp.int32, (tokens, tokens), 0)
        == lax.broadcasted_iota(jnp.int32, (tokens, tokens), 1), 1.0, 0.0,
    ).astype(BF)

    def weigh(z):
        slots = lax.broadcasted_iota(jnp.int32, (rows, tokens), 0).astype(F32)
        m = meta_all[z]
        pick = jnp.where(slots == m[0:1], m[2:3], 0.0) + jnp.where(slots == m[1:2], m[3:4], 0.0)
        mix[z] = lax.dot_general(
            eye, pick.astype(BF), (((1,), (1,)), ((), ())), preferred_element_type=F32
        ).astype(BF)

    each(ndp, weigh)

    if n_a:
        turn_a(n_a - 1)

    def back_a(i):
        cols = span(i)
        landed(from_l.at[:, :, :, cols], fl.at[i])
        landed(from_r.at[:, :, :, cols], fr.at[i])

        def add(e):
            some = pl.ds(e * 4, 4)
            flat = (4 * cap, width)
            total = own_a[dp, some, :, :, cols].reshape(flat).astype(F32)
            total = total + from_l[some, :, :, cols].reshape(flat).astype(F32)
            total = total + from_r[some, :, :, cols].reshape(flat).astype(F32)
            send_a[some, :, :, cols] = total.astype(BF).reshape(4, cap // 2, 2, width)

        each(nseq // 4, add)
        ret_a[me, :, :, cols] = send_a[me, :, :, cols]

        def go(d, carry):
            e = lax.rem(me + HOP * d, nseq)
            push(send_a.at[e, :, :, cols], ret_a.at[me, :, :, cols], as_, ar.at[i], dp, e)
            return carry

        lax.fori_loop(1, nseq, go, 0)

    def mix_b(i):
        cols = span(i)
        landed(ret_b.at[:, pl.ds(0, nseq - 1), :, :, cols], br.at[i])

        def part(z):
            block = ret_b[z, :, :, :, cols].reshape(rows, width)
            sums[z, :, cols] = jnp.dot(mix[z], block, preferred_element_type=F32).astype(BF)

        each(ndp, part)
        for j in near:
            z = lax.rem(dp + j, ndp)
            push(sums.at[z, :, cols], got.at[dp, :, cols], ss, sr.at[i], z, me)

    interleave(n_b, n_a, mix_b, back_a)

    def end_a(i):
        cols = span(i)
        landed(ret_a.at[pl.ds(0, nseq - 1), :, :, cols], ar.at[i])
        block = ret_a[:, :, :, cols].reshape(rows, width)
        mixed = jnp.dot(mix[dp], block, preferred_element_type=F32)
        out[:, cols] = (base[:, cols].astype(F32) + mixed).astype(BF)

    def end_b(i):
        cols, there = span(i), span(i, ca)
        landed(got.at[pl.ds(0, ndp - 1), :, cols], sr.at[i])
        total = sums[dp, :, cols].astype(F32)
        for j in range(1, ndp):
            total = total + got[lax.rem(dp + j, ndp), :, cols].astype(F32)
        out[:, there] = (base[:, there].astype(F32) + total).astype(BF)

    interleave(n_b, n_a, end_b, end_a)
    if n_a:
        landed(own_a.at[0], zs)
        landed(own_a.at[pl.ds(0, 2)], fs)
        landed(send_a.at[pl.ds(0, nseq - 1)], as_)
    if n_b:
        landed(part_b.at[:, pl.ds(0, nseq - 1)], bs)
        landed(sums.at[pl.ds(0, ndp - 1)], ss)


def experts(
    normed, base, q, k, v, g, run, factor, back, meta, w_in, w_out, ndp, nseq, cap, split
):
    tokens, model = normed.shape
    hidden = w_in.shape[1]
    n_a, n_b, width = split
    rows = nseq * cap
    ca, cb = n_a * width, n_b * width
    cfg = (ndp, nseq, cap, width, n_a, n_b)
    dma = pltpu.SemaphoreType.DMA
    whole = pl.BlockSpec(memory_space=pltpu.VMEM)
    away = pl.BlockSpec(memory_space=pl.ANY)
    hid, meta_all, key_out, value_out = pl.pallas_call(
        functools.partial(dispatch_kernel, cfg),
        out_shape=(
            jax.ShapeDtypeStruct((ndp * rows, hidden), BF),
            jax.ShapeDtypeStruct((ndp, 8, tokens), F32),
            jax.ShapeDtypeStruct((tokens, model), BF),
            jax.ShapeDtypeStruct((tokens, model), BF),
        ),
        in_specs=[whole, whole] + [away] * 5 + [whole] * 3,
        out_specs=(whole,) * 4,
        scratch_shapes=[
            vmem(ndp, nseq, cap // 2, 2, model),
            vmem(nseq, cap // 2, 2, max(ca, 128)),
            vmem(ndp, nseq, cap // 2, 2, max(cb, 128)),
            vmem(ndp, tokens, max(cb, 128)),
            vmem(ndp, 8, tokens, kind=F32),
            vmem(ndp, rows, tokens),
            vmem(hidden, model),
            vmem(ndp * rows, hidden, kind=F32),
            vmem(*back.shape),
            vmem(tokens, model),
            vmem(tokens, model),
            vmem(tokens, model),
            vmem(tokens, model),
            dma, dma((4,)), dma, dma, dma, dma((max(n_b, 1),)), dma, dma((max(n_a, 1),)),
            dma, dma((max(n_b, 1),)), dma, dma((max(n_a, 1),)), dma((max(n_a, 1),)),
            dma, dma((max(n_a, 1),)), dma((max(n_a, 1),)), dma, dma,
        ],
        compiler_params=pltpu.CompilerParams(
            collective_id=1, has_side_effects=True, vmem_limit_bytes=62 << 20
        ),
        name="dispatch",
    )(normed, meta, w_in, q, k, v, g, run, factor, back)
    layer_out = pl.pallas_call(
        functools.partial(combine_kernel, cfg),
        out_shape=jax.ShapeDtypeStruct((tokens, model), BF),
        in_specs=[whole, whole, away, whole],
        out_specs=whole,
        scratch_shapes=[
            vmem(ndp, nseq, cap // 2, 2, max(ca, 128)),
            vmem(ndp, nseq, cap // 2, 2, max(cb, 128)),
            vmem(nseq // 2, cap // 2, 2, max(ca, 128)),
            vmem(nseq // 2, cap // 2, 2, max(ca, 128)),
            vmem(nseq, cap // 2, 2, max(ca, 128)),
            vmem(nseq, cap // 2, 2, max(ca, 128)),
            vmem(nseq, cap // 2, 2, max(ca, 128)),
            vmem(nseq, cap // 2, 2, max(ca, 128)),
            vmem(ndp, nseq, cap // 2, 2, max(cb, 128)),
            vmem(ndp, tokens, max(cb, 128)),
            vmem(ndp, tokens, max(cb, 128)),
            vmem(ndp, tokens, rows),
            vmem(hidden, model),
            dma((n_a + n_b,)), dma, dma((max(n_a, 1),)), dma((max(n_a, 1),)),
            dma, dma((max(n_a, 1),)), dma((max(n_a, 1),)), dma, dma((max(n_b, 1),)),
            dma, dma((max(n_a, 1),)), dma, dma((max(n_b, 1),)),
        ],
        compiler_params=pltpu.CompilerParams(
            collective_id=2, has_side_effects=True, vmem_limit_bytes=62 << 20
        ),
        name="combine",
    )(hid, meta_all, w_out, base)
    return layer_out, key_out, value_out


norm_eps = 1e-06
TOP = 2
SPLIT = (5, 3, 512)


def on_device(
    queries, keys, values, log_decay, attn_grad, norm_gain, route_ids, route_weights, grad_exponent,
    w_in, w_out,
):
    length, width = queries.shape[1:]
    ndp, nseq = lax.axis_size("dp"), lax.axis_size("seq")
    heads = log_decay.shape[1]
    head = width // heads
    cap = max(2, TOP * length * 5 // (4 * nseq))
    factor = jnp.broadcast_to(jnp.exp2(grad_exponent.astype(F32))[:, None], (heads, head))
    args = (queries, keys, values, attn_grad)
    ids = jnp.swapaxes(route_ids, 1, 2)
    weights = jnp.swapaxes(route_weights, 1, 2)
    attn_out, normed, back, run, meta = attention(
        *args, log_decay, norm_gain[None], ids, weights, ndp, nseq, head, cap
    )
    layer_out, key_out, value_out = experts(
        normed, attn_out, *args, run, factor, back, meta, w_in, w_out, ndp, nseq, cap, SPLIT
    )
    return (layer_out[None], key_out[None], value_out[None])


def solution(mesh):
    rows = P("dp", "seq", None)
    placed = (
        rows, rows, rows, P("dp", None, "seq"), rows, P(), rows, rows, P(),
        P("seq", "dp", None), P("seq", "dp", None),
    )
    return jax.shard_map(
        on_device, mesh=mesh, in_specs=placed, out_specs=(rows, rows, rows), check_vma=False
    )
```
